256 devices in a mesh: enc: 8 (over z), bin: 16 (over y_hi, x, core), off: 2 (over y_lo).
Axes of the slice: x: 4, y: 4 (y_hi: 2, y_lo: 2; y = y_hi * 2 + y_lo), z: 8, core: 2. Of those that a mesh axis runs over, the one named last changes fastest.
Arguments:
- encoder_in: bfloat16 [512, 6144], P(('bin', 'off'), 'enc'), may hold values from -6 to 6
- gain_enc: float32 [512], P(('bin', 'off')), may hold values from 0.1 to 1.9
- conv_one: bfloat16 [3, 512, 512], P(None, ('bin', 'off')), may hold values from -0.15625 to 0.15625
- proj_weight: bfloat16 [2, 512, 32], P(None, ('bin', 'off')), may hold values from -0.25 to 0.25
- conv_two: bfloat16 [9, 32, 32], replicated, may hold values from -0.375 to 0.375
- head_weight: float32 [32], replicated, may hold values from -1 to 1
- target: bfloat16 [6144, 2048], P('bin', ('enc', 'off')), may hold values from -8 to 8
- valid_bins: int32 [6144], replicated, may hold values 0 or 1
- offset_limit: int32 [6144], replicated, may hold values from 1024 to 2048
- dilations: int32 [2], replicated, may hold values from 1 to 8, as said below
Outputs:
- prediction: float32 [6144, 2048], P('bin', ('enc', 'off'))
- loss_mean: float32 [1], replicated
- grad_conv_two: float32 [9, 32, 32], replicated
- grad_proj: float32 [2, 512, 32], P(None, ('bin', 'off'))
- grad_conv_one: float32 [3, 512, 512], P(None, ('bin', 'off'), 'enc')
The draws below stay inside these ranges and needn't reach their ends.
Inputs may be any that keep to these rules, and one draw needn't show every extreme that they name: dilations[0] is the dilation of the 1-D layer and dilations[1] that of the 2-D layer; one of the two equals 8, the other is smaller.
All inputs are finite; a program needn't handle non-finite values.
Results may differ from the reference program's by a relative error of at most 0.0013.
The reference program's roundings to bfloat16 on the way (of `activ`, `hidden`, `embed`, `band_act`, `dres`, `grad_embed` and `dhidden`) count: a program that leaves them out, or rounds other values in their place, can miss the bound.
Values may be sent and summed in bfloat16 or wider, within the bound.
No kernel may reach another device: no remote copies, remote signals or barrier semaphores. Data moves between devices by JAX's collectives and lax.ppermute only.
A program may use at most 192 MiB of HBM per device.

```python
import jax
import jax.numpy as jnp
from jax import lax

C1 = 512
C2 = 32
BAND_TILE_BINS = 384
KD = 128
LARGEST_DILATION = 8
L = 6144
K = 2048
N_ENC = 8
N_BIN = 16
N_OFF = 2


def draw_dilations(key, part):
    first, second = jax.random.split(jax.random.fold_in(key, 11))
    other = jax.random.randint(first, (), 1, LARGEST_DILATION).astype(jnp.int32)
    order = jax.random.randint(second, (), 0, 2)
    largest = jnp.full((), LARGEST_DILATION, jnp.int32)
    return jnp.where(order == 1, jnp.stack([largest, other]), jnp.stack([other, largest])).astype(jnp.int32)


def draw_target(key, part):
    offsets = jnp.arange(K, dtype=jnp.float32) / K
    scale = 0.5 + 1.5 * offsets
    values = jax.random.normal(jax.random.fold_in(key, 23), (L, K), jnp.float32) * scale[None, :]
    return jnp.clip(values, -8.0, 8.0).astype(jnp.bfloat16)


def plant(entries, key, low, high):
    longest = entries.shape.index(max(entries.shape))
    spots = []
    for shift in (0, 1):
        where = [jax.random.randint(jax.random.fold_in(key, axis), (), 0, length) for axis, length in enumerate(entries.shape)]
        where[longest] = (where[longest] + shift) % entries.shape[longest]
        spots.append(tuple(where))
    return entries.at[spots[0]].set(low).at[spots[1]].set(high)


def shard_levels(key, dims, pieces, low, top_value):
    def one(position, parts):
        steps = jax.random.uniform(jax.random.fold_in(jax.random.fold_in(key, 6), position), (parts,), jnp.float32, low / len(pieces), top_value / len(pieces))
        return jnp.repeat(jnp.exp(steps), dims[position] // parts).reshape((-1,) + (1,) * (len(dims) - position - 1))

    gain = one(*pieces[0])
    for cut in pieces[1:]:
        gain = gain * one(*cut)
    return gain


def scatter_about(stream_key, extent, spread, reach, cuts=(), kind=jnp.bfloat16):
    array = spread * jax.random.normal(stream_key, extent, jnp.float32)
    if cuts:
        array = array * shard_levels(stream_key, extent, cuts, -0.22, 0.18)
    return jnp.clip(array, -reach, reach).astype(kind)


def setup_inputs(seed: int = 0) -> dict:
    splits = jax.random.split(jax.random.key(seed), 11)
    encoder_in = scatter_about(splits[0], (C1, L), 1.0, 6.0, ((0, 32), (1, 8)))
    gain_enc = jnp.clip(1.0 + 0.18 * jax.random.normal(splits[1], (C1,), jnp.float32), 0.1, 1.9)
    conv_one = scatter_about(splits[2], (3, C1, C1), (3 * C1) ** -0.5, 0.15625, ((1, 32),))
    proj_weight = scatter_about(splits[3], (2, C1, C2), C1 ** -0.5, 0.25, ((1, 32),))
    conv_two = scatter_about(splits[4], (9, C2, C2), (9 * C2) ** -0.5, 0.375)
    head_weight = scatter_about(splits[5], (C2,), C2 ** -0.5, 1.0, (), jnp.float32)
    target = draw_target(jax.random.fold_in(splits[10], 71), 0)
    valid_bins = plant((jax.random.randint(splits[7], (L,), 0, 8) < 7).astype(jnp.int32), jax.random.fold_in(splits[7], 1), 0, 1)
    offset_limit = plant(jax.random.randint(splits[8], (L,), K // 2, K + 1), jax.random.fold_in(splits[8], 1), K // 2, K).astype(jnp.int32)
    dilations = draw_dilations(jax.random.fold_in(splits[10], 71), 0)
    return {"encoder_in": encoder_in, "gain_enc": gain_enc, "conv_one": conv_one, "proj_weight": proj_weight, "conv_two": conv_two, "head_weight": head_weight, "target": target, "valid_bins": valid_bins, "offset_limit": offset_limit, "dilations": dilations}


def rounded(values):
    return lax.optimization_barrier(values.astype(jnp.bfloat16)).astype(jnp.float32)


def indices(*values):
    return tuple(jnp.asarray(value).astype(jnp.int32) for value in values)


def hankel(window, tile_rows, tile_cols):
    chans = window.shape[0]
    width = tile_rows + tile_cols
    base = window[:, :width - 1]
    tiled = jnp.broadcast_to(base[:, None, :], (chans, tile_rows, width - 1)).reshape(chans, tile_rows * (width - 1))
    tiled = jnp.pad(tiled, ((0, 0), (0, tile_rows)))
    return tiled.reshape(chans, tile_rows, width)[:, :, :tile_cols]


def diagonal_sums(tile):
    chans, tile_rows, tile_cols = tile.shape
    width = tile_rows + tile_cols
    padded_input = jnp.pad(tile, ((0, 0), (0, 0), (0, tile_rows)))
    flat = padded_input.reshape(chans, tile_rows * width)[:, :tile_rows * (width - 1)]
    return jnp.sum(flat.reshape(chans, tile_rows, width - 1), axis=1)


def count_cells(valid_bins, offset_limit):
    sequence_length = valid_bins.shape[0]
    running = jnp.concatenate([jnp.zeros((1,), jnp.int32), jnp.cumsum(valid_bins).astype(jnp.int32)])
    places = jnp.arange(sequence_length, dtype=jnp.int32)
    farthest = jnp.minimum(places + offset_limit.astype(jnp.int32), sequence_length)
    inside = jnp.take(running, farthest) - jnp.take(running, places)
    return jnp.sum(valid_bins.astype(jnp.int32) * inside).astype(jnp.float32)


def reference(encoder_in, gain_enc, conv_one, proj_weight, conv_two, head_weight, target, valid_bins, offset_limit, dilations):
    highest = lax.Precision.HIGHEST
    first_dilation = dilations[0].astype(jnp.int32)
    second_dilation = dilations[1].astype(jnp.int32)
    sequence_length = BAND_TILE_BINS * N_BIN
    window_extent = KD * N_ENC * N_OFF
    second_channels = conv_two.shape[1]
    activ = rounded(jax.nn.gelu(gain_enc[:, None] * encoder_in.astype(jnp.float32)))
    padded_input = jnp.pad(activ, ((0, 0), (LARGEST_DILATION, LARGEST_DILATION)))
    section_list = [lax.dynamic_slice_in_dim(padded_input, indices(LARGEST_DILATION + (kernel_tap_index - 1) * first_dilation)[0], sequence_length, 1) for kernel_tap_index in range(3)]
    conv_out = jnp.zeros((conv_one.shape[1], sequence_length), jnp.float32)
    for kernel_tap_index in range(3):
        conv_out = conv_out + jnp.dot(conv_one[kernel_tap_index].astype(jnp.float32), section_list[kernel_tap_index], precision=highest)
    hidden = rounded(encoder_in.astype(jnp.float32) + conv_out)
    embed = rounded(jnp.einsum("kce,ci->kei", proj_weight.astype(jnp.float32), hidden, precision=highest))
    border_width = 2 * LARGEST_DILATION
    wide_rows = BAND_TILE_BINS + 4 * LARGEST_DILATION
    middle_rows = BAND_TILE_BINS + 2 * LARGEST_DILATION
    near_ext = jnp.pad(embed[0], ((0, 0), (border_width, border_width + BAND_TILE_BINS)))
    far_ext = jnp.pad(embed[1], ((0, 0), (border_width, window_extent + border_width + BAND_TILE_BINS)))
    mask_ext = jnp.pad(valid_bins.astype(jnp.float32), (LARGEST_DILATION, window_extent + LARGEST_DILATION + BAND_TILE_BINS))
    limit_ext = jnp.pad(offset_limit.astype(jnp.int32), (LARGEST_DILATION, LARGEST_DILATION + BAND_TILE_BINS))
    target_ext = jnp.pad(target.astype(jnp.float32), ((LARGEST_DILATION, LARGEST_DILATION + BAND_TILE_BINS), (0, 0)))
    denom = 1.0 + count_cells(valid_bins, offset_limit)
    weights_two = conv_two.astype(jnp.float32)
    shifts = [(bin_displacement, offset_displacement) for bin_displacement in (-1, 0, 1) for offset_displacement in (-1, 0, 1)]
    offs_ids = jnp.arange(window_extent, dtype=jnp.int32)

    def block(carry, block_index):
        buffer, grad_band, error_sum = carry
        start = (block_index * BAND_TILE_BINS).astype(jnp.int32)
        row_ids = start - border_width + jnp.arange(wide_rows, dtype=jnp.int32)
        inside = ((row_ids >= 0) & (row_ids < sequence_length)).astype(jnp.float32)
        near_rows = lax.dynamic_slice_in_dim(near_ext, start, wide_rows, 1)
        far_rows = hankel(lax.dynamic_slice_in_dim(far_ext, start, wide_rows + window_extent, 1), wide_rows, window_extent)
        pair_sum = near_rows[:, :, None] + far_rows
        band_act = rounded(jnp.maximum(pair_sum, 0.0) * inside[None, :, None])
        activation_padded = jnp.pad(band_act, ((0, 0), (0, 0), (LARGEST_DILATION, LARGEST_DILATION)))
        band_conv = jnp.zeros((second_channels, middle_rows, window_extent), jnp.float32)
        for kernel_tap_index, (bin_displacement, offset_displacement) in enumerate(shifts):
            section_index = lax.dynamic_slice(activation_padded, indices(0, LARGEST_DILATION + bin_displacement * second_dilation, LARGEST_DILATION + offset_displacement * second_dilation), (second_channels, middle_rows, window_extent))
            band_conv = band_conv + jnp.einsum("ef,exy->fxy", weights_two[kernel_tap_index], section_index, precision=highest)
        pair_mid = pair_sum[:, LARGEST_DILATION:LARGEST_DILATION + middle_rows]
        resid = pair_mid + band_conv
        pred_mid = jnp.sum(head_weight[:, None, None] * jnp.maximum(resid, 0.0), axis=0)
        mask_rows = lax.dynamic_slice_in_dim(mask_ext, start, middle_rows)
        mask_far = hankel(lax.dynamic_slice_in_dim(mask_ext, start, middle_rows + window_extent)[None, :], middle_rows, window_extent)[0]
        limit_rows = lax.dynamic_slice_in_dim(limit_ext, start, middle_rows)
        weight = mask_rows[:, None] * mask_far * (offs_ids[None, :] < limit_rows[:, None]).astype(jnp.float32)
        target_rows = lax.dynamic_slice_in_dim(target_ext, start, middle_rows, 0)
        differ = pred_mid - target_rows
        dpred = 2.0 * weight * differ / denom
        dres = rounded(head_weight[:, None, None] * dpred[None] * (resid > 0.0).astype(jnp.float32))
        own_weight = weight[LARGEST_DILATION:LARGEST_DILATION + BAND_TILE_BINS]
        own_differ = differ[LARGEST_DILATION:LARGEST_DILATION + BAND_TILE_BINS]
        error_sum = error_sum + jnp.sum(own_weight * own_differ * own_differ)
        dres_own = dres[:, LARGEST_DILATION:LARGEST_DILATION + BAND_TILE_BINS]
        residual_grad_padded = jnp.pad(dres, ((0, 0), (0, 0), (LARGEST_DILATION, LARGEST_DILATION)))
        dact = jnp.zeros((second_channels, BAND_TILE_BINS, window_extent), jnp.float32)
        for kernel_tap_index, (bin_displacement, offset_displacement) in enumerate(shifts):
            activation_section = lax.dynamic_slice(activation_padded, indices(0, border_width + bin_displacement * second_dilation, LARGEST_DILATION + offset_displacement * second_dilation), (second_channels, BAND_TILE_BINS, window_extent))
            grad_band = grad_band.at[kernel_tap_index].add(jnp.einsum("exy,fxy->ef", activation_section, dres_own, precision=highest))
            residual_grad_section = lax.dynamic_slice(residual_grad_padded, indices(0, LARGEST_DILATION - bin_displacement * second_dilation, LARGEST_DILATION - offset_displacement * second_dilation), (second_channels, BAND_TILE_BINS, window_extent))
            dact = dact + jnp.einsum("ef,fxy->exy", weights_two[kernel_tap_index], residual_grad_section, precision=highest)
        pair_own = pair_sum[:, border_width:border_width + BAND_TILE_BINS]
        dpair = dres_own + dact * (pair_own > 0.0).astype(jnp.float32)
        near_grad = jnp.sum(dpair, axis=2)
        far_grad = diagonal_sums(dpair)
        old_near = lax.dynamic_slice(buffer, indices(0, 0, start), (1, second_channels, BAND_TILE_BINS))
        buffer = lax.dynamic_update_slice(buffer, old_near + near_grad[None], indices(0, 0, start))
        old_far = lax.dynamic_slice(buffer, indices(1, 0, start), (1, second_channels, BAND_TILE_BINS + window_extent - 1))
        buffer = lax.dynamic_update_slice(buffer, old_far + far_grad[None], indices(1, 0, start))
        return (buffer, grad_band, error_sum), pred_mid[LARGEST_DILATION:LARGEST_DILATION + BAND_TILE_BINS]

    init = (jnp.zeros((2, second_channels, sequence_length + window_extent + BAND_TILE_BINS), jnp.float32), jnp.zeros((9, second_channels, second_channels), jnp.float32), jnp.zeros((), jnp.float32))
    (buffer, grad_band, error_sum), preds = lax.scan(block, init, jnp.arange(sequence_length // BAND_TILE_BINS, dtype=jnp.int32))
    prediction = preds.reshape(sequence_length, window_extent)
    grad_embed = rounded(buffer[:, :, :sequence_length])
    dhidden = rounded(jnp.einsum("kce,kei->ci", proj_weight.astype(jnp.float32), grad_embed, precision=highest))
    grad_proj = jnp.einsum("ci,kei->kce", hidden, grad_embed, precision=highest)
    grad_conv_one = jnp.stack([jnp.einsum("ji,ci->jc", dhidden, section_list[kernel_tap_index], precision=highest) for kernel_tap_index in range(3)])
    loss_mean = (error_sum / denom).reshape(1)
    return prediction, loss_mean, grad_band, grad_proj, grad_conv_one
```

```python
import jax
import jax.numpy as jnp
from jax import lax
from jax.experimental import pallas as pl
from jax.experimental.pallas import tpu as pltpu
from jax.sharding import PartitionSpec as P

LARGEST_DILATION = 8
HALO = LARGEST_DILATION
EDGE = 2 * LARGEST_DILATION
F32 = jnp.float32
BF16 = jnp.bfloat16
MASKED = -1e38
GROUP = ("bin", "off")
EVERY = ("enc", "bin", "off")


def with_halo(cells, axis, dim, width):
    count = lax.axis_size(axis)
    ends = count - 1
    head = lax.slice_in_dim(cells, 0, width, axis=dim)
    tail = lax.slice_in_dim(cells, cells.shape[dim] - width, cells.shape[dim], axis=dim)
    return jnp.concatenate(
        [
            lax.ppermute(tail, axis, [(i, (i + 1) % count) for i in range(ends)]),
            cells,
            lax.ppermute(head, axis, [((i + 1) % count, i) for i in range(ends)]),
        ],
        axis=dim,
    )


def exchange(array, axis):
    return lax.all_to_all(array, axis, 0, 0, tiled=True)


def from_everyone(array, axis):
    return exchange(jnp.broadcast_to(array[None], (lax.axis_size(axis), *array.shape)), axis)


def pieces(x, shift):
    return [
        pltpu.roll(x[:, start : start + 128], shift, 1) for start in range(0, x.shape[1], 128)
    ]


def moved_right(x, shift):
    parts = pieces(x, shift)
    edge = lax.broadcasted_iota(jnp.int32, parts[0].shape, 1) < shift
    return jnp.concatenate(
        [jnp.where(edge, parts[k - 1], parts[k]) for k in range(len(parts))], axis=1
    )


def moved_left(x, shift):
    parts = pieces(x, 128 - shift)
    edge = lax.broadcasted_iota(jnp.int32, parts[0].shape, 1) < 128 - shift
    return jnp.concatenate(
        [jnp.where(edge, parts[k], parts[(k + 1) % len(parts)]) for k in range(len(parts))],
        axis=1,
    )


def count_body(flags_ref, flags_t_ref, limit_ref, out_ref):
    total = limit_ref.shape[1]
    chunk = 512
    flags_t = flags_t_ref[...].astype(BF16)
    high = flags_t.shape[1]
    place = lax.broadcasted_iota(jnp.int32, (128, 128), 0)
    other = lax.broadcasted_iota(jnp.int32, (128, 128), 1)
    before = jnp.where(other < place, 1.0, 0.0).astype(BF16)
    row_h = lax.broadcasted_iota(jnp.int32, (high, high), 0)
    col_h = lax.broadcasted_iota(jnp.int32, (high, high), 1)
    before_h = jnp.where(row_h < col_h, 1.0, 0.0).astype(BF16)
    inner = jnp.dot(before, flags_t, preferred_element_type=F32)
    outer = jnp.sum(jnp.dot(flags_t, before_h, preferred_element_type=F32), axis=0, keepdims=True)
    table = inner + outer
    table_hi = jnp.floor(table * (1.0 / 128.0))
    table_lo = (table - 128.0 * table_hi).astype(BF16)
    table_hi = table_hi.astype(BF16)
    row_of = lax.broadcasted_iota(jnp.int32, (high, chunk), 0)
    lane_of = lax.broadcasted_iota(jnp.int32, (128, chunk), 0)
    ids = lax.broadcasted_iota(jnp.int32, (1, chunk), 1)

    def looked_up(where):
        picks = jnp.where(row_of == lax.shift_right_logical(where, 7), 1.0, 0.0).astype(BF16)
        found = 128.0 * jnp.dot(table_hi, picks, preferred_element_type=F32) + jnp.dot(
            table_lo, picks, preferred_element_type=F32
        )
        return jnp.sum(
            jnp.where(lane_of == (where & 127), found, 0.0), axis=0, keepdims=True
        )

    acc = jnp.zeros((1, chunk), F32)
    for start in range(0, total, chunk):
        here = ids + start
        far = jnp.minimum(here + limit_ref[:, start : start + chunk], total)
        inside = looked_up(far) - looked_up(here)
        acc = acc + flags_ref[:, start : start + chunk].astype(F32) * inside
    out_ref[...] = jnp.broadcast_to(jnp.sum(acc, axis=1, keepdims=True), out_ref.shape)


def count_cells(valid_bins, offset_limit):
    total = valid_bins.shape[0]
    rows = -(-(total // 128 + 1) // 128) * 128
    flags = jnp.zeros((rows, 128), jnp.int32)
    flags = lax.dynamic_update_slice(flags, valid_bins.reshape(total // 128, 128), (0, 0))
    return pl.pallas_call(
        count_body, out_shape=jax.ShapeDtypeStruct((8, 128), F32), name="count"
    )(valid_bins[None], flags.astype(F32).T, offset_limit[None])


def band_body(
    info_ref,
    embed_ref,
    flag_near_ref,
    flag_far_ref,
    limit_ref,
    target_ref,
    fwd_ref,
    back_ref,
    head_ref,
    count_ref,
    pred_ref,
    near_out,
    far_out,
    grad_out,
    err_out,
    lines,
    parts,
    dress,
    owns,
    weights,
    goals,
):
    wide = limit_ref.shape[1]
    chans = near_out.shape[0]
    cols, rows = pred_ref.shape
    steps = cols + 2 * EDGE
    first_mid, last_mid = HALO, steps - HALO
    dilation = info_ref[0]
    offs_start = info_ref[1]
    row_start = info_ref[2]
    extent = info_ref[3]
    length = info_ref[4]
    wide_far = embed_ref.shape[1]
    turn = 448
    lane = lax.broadcasted_iota(jnp.int32, (1, wide), 1)
    bins = row_start + jnp.where(lane < turn, lane, lane - wide)
    near = jnp.where(
        (bins >= 0) & (bins < length), moved_left(moved_left(embed_ref[:chans].astype(F32), EDGE)[:, :wide], EDGE), MASKED
    )
    near_of = (
        moved_right(near, dilation).astype(BF16),
        near.astype(BF16),
        moved_left(near, dilation).astype(BF16),
    )
    flag_near = moved_left(jnp.broadcast_to(flag_near_ref[...], (8, wide)), EDGE)
    limit = moved_left(jnp.broadcast_to(limit_ref[...], (8, wide)), EDGE)
    goals[...] = moved_left(target_ref[...], EDGE)
    far = moved_left(embed_ref[chans:].astype(F32), HALO).astype(BF16)
    flags = moved_left(jnp.broadcast_to(flag_far_ref[...], (8, wide_far)), HALO)
    tiles = wide // 128
    tiles_far = wide_far // 128
    lane_tile = lax.broadcasted_iota(jnp.int32, (chans, 128), 1)
    before_turn = lane_tile < turn % 128

    def shifted(rolled, shift, extra, last_only):
        keep = last_only < 128 - shift

        def part(k):
            return jnp.where(keep, rolled[k % tiles_far], rolled[(k + 1) % tiles_far])

        out = [part(k + extra) for k in range(tiles)]
        out[-1] = jnp.where(last_only < turn % 128, out[-1], part(tiles + extra))
        return jnp.concatenate(out, axis=1)

    def make_line(shift, extra):
        turned = (128 - shift) & 127
        rolled = pieces(far, turned)
        rolled_flags = pieces(flags, turned)
        for more in range(extra):
            u = shift + 128 * more
            lines[u] = shifted(rolled, shift, more, lane_tile)
            flag = shifted(rolled_flags, shift, more, lane_tile[:8])
            offset = offs_start + u - HALO - EDGE
            offset = jnp.where(offset >= 0, offset, extent).astype(F32)
            weights[u] = jnp.where(limit > offset, flag_near * flag, 0.0)

    total_lines = steps + 2 * HALO
    both = total_lines - 128

    @pl.loop(0, both, unroll=8)
    def _(shift):
        make_line(shift, 2)

    @pl.loop(both, 128, unroll=8)
    def _(shift):
        make_line(shift, 1)

    def act_of(t, tap, width):
        line = lines[t + HALO + (tap - 1) * dilation, :, :width]
        return jnp.maximum(near_of[tap][:, :width] + line, jnp.zeros((), BF16))

    fwd = fwd_ref[...]

    @pl.loop(0, steps, unroll=40)
    def _(t):
        stacked = jnp.concatenate([act_of(t, tap, wide) for tap in range(3)], axis=0)
        parts[t] = jnp.dot(fwd, stacked, preferred_element_type=F32)

    @pl.when(offs_start == 0)
    def _():
        @pl.loop(0, EDGE)
        def _(t):
            parts[t] = jnp.zeros((3 * chans, wide), F32)

    @pl.when(offs_start + cols == extent)
    def _():
        @pl.loop(steps - EDGE, steps)
        def _(t):
            parts[t] = jnp.zeros((3 * chans, wide), F32)

    owns[:EDGE] = jnp.zeros((EDGE, chans, rows), BF16)
    owns[steps - EDGE :] = jnp.zeros((EDGE, chans, rows), BF16)
    head = jnp.broadcast_to(head_ref[...], (chans, wide))
    scale = 2.0 / (1.0 + count_ref[0:1, 0:1])

    def make_dres(t, err, own):
        conv = (
            parts[t - dilation, :chans]
            + parts[t, chans : 2 * chans]
            + parts[t + dilation, 2 * chans :]
        )
        resid = (near + lines[t + HALO].astype(F32)) + conv
        pred = jnp.sum(head * jnp.maximum(resid, 0.0), axis=0, keepdims=True)
        differ = pred - goals[pl.ds(t - HALO, 1)]
        weighted = weights[t + HALO, 0:1] * differ
        dres = jnp.where(resid > 0.0, head * (weighted * scale), 0.0).astype(BF16)
        dress[t] = dres
        if own:
            owns[t] = dres[:, :rows]
            pred_ref[pl.ds(t - EDGE, 1)] = pred[:, :rows]
            err = err + (weighted * differ)[:, :rows]
        return err

    err = jnp.zeros((1, rows), F32)
    err = lax.fori_loop(first_mid, EDGE, lambda t, e: make_dres(t, e, False), err, unroll=4)
    err = lax.fori_loop(EDGE, steps - EDGE, lambda t, e: make_dres(t, e, True), err, unroll=8)
    err = lax.fori_loop(
        steps - EDGE, last_mid, lambda t, e: make_dres(t, e, False), err, unroll=4
    )
    err_out[...] = jnp.broadcast_to(jnp.sum(err, axis=1, keepdims=True), err_out.shape)
    back = back_ref[...]

    @pl.loop(first_mid, last_mid, unroll=36)
    def _(t):
        dres = dress[t]
        stacked = jnp.concatenate(
            [
                moved_left(dres, dilation)[:, :rows],
                dres[:, :rows],
                moved_right(dres, dilation)[:, :rows],
            ],
            axis=0,
        )
        parts[t, :, :rows] = jnp.dot(back, stacked, preferred_element_type=F32)

    bunch = 8

    def make_grads(n, carry):
        near_sum, far_sum = carry
        far_sum = moved_right(far_sum, bunch)
        for k in range(bunch):
            t = steps - EDGE - bunch - n * bunch + k
            dact = (
                parts[t + dilation, :chans, :rows]
                + parts[t, chans : 2 * chans, :rows]
                + parts[t - dilation, 2 * chans :, :rows]
            )
            act = act_of(t, 1, rows).astype(F32)
            dpair = owns[t].astype(F32) + jnp.where(act > 0.0, dact, 0.0)
            near_sum = near_sum + dpair
            dpair = jnp.concatenate([dpair, jnp.zeros((chans, wide - rows), F32)], axis=1)
            far_sum = far_sum + (moved_right(dpair, k) if k else dpair)
        return near_sum, far_sum

    near_sum, far_sum = lax.fori_loop(
        0,
        cols // bunch,
        make_grads,
        (jnp.zeros((chans, rows), F32), jnp.zeros((chans, wide), F32)),
    )
    near_out[...] = near_sum
    far_out[...] = far_sum
    grad_out[...] = jnp.zeros((3 * chans, 3 * chans), F32)

    def add_weight_grads(first, batch):
        left = jnp.concatenate(
            [
                jnp.concatenate([act_of(first + k, tap, rows) for tap in range(3)], axis=0)
                for k in range(batch)
            ],
            axis=1,
        )
        right = jnp.concatenate(
            [
                jnp.concatenate([owns[first + k + move * dilation] for k in range(batch)], axis=1)
                for move in (1, 0, -1)
            ],
            axis=0,
        )
        grad_out[...] += lax.dot_general(
            left, right, (((1,), (1,)), ((), ())), preferred_element_type=F32
        )

    batch = 16

    @pl.loop(0, cols // batch)
    def _(n):
        add_weight_grads(EDGE + n * batch, batch)

    @pl.when(offs_start > 0)
    def _():
        add_weight_grads(first_mid, HALO)

    @pl.when(offs_start + cols < extent)
    def _():
        add_weight_grads(steps - EDGE, HALO)


def band(info, embed, flag_near, flag_far, limit, target, fwd, back, head, count, rows, cols):
    chans = embed.shape[0] // 2
    wide = limit.shape[1]
    steps = cols + 2 * EDGE
    vmem = pl.BlockSpec(memory_space=pltpu.VMEM)
    return pl.pallas_call(
        band_body,
        out_shape=(
            jax.ShapeDtypeStruct((cols, rows), F32),
            jax.ShapeDtypeStruct((chans, rows), F32),
            jax.ShapeDtypeStruct((chans, wide), F32),
            jax.ShapeDtypeStruct((3 * chans, 3 * chans), F32),
            jax.ShapeDtypeStruct((8, 128), F32),
        ),
        in_specs=[pl.BlockSpec(memory_space=pltpu.SMEM)] + [vmem] * 9,
        out_specs=(vmem,) * 5,
        scratch_shapes=[
            pltpu.VMEM((steps + 2 * HALO, chans, wide), BF16),
            pltpu.VMEM((steps, 3 * chans, wide), F32),
            pltpu.VMEM((steps, chans, wide), BF16),
            pltpu.VMEM((steps, chans, rows), BF16),
            pltpu.VMEM((steps + 2 * HALO, 8, wide), F32),
            pltpu.VMEM((steps - 2 * HALO, wide), F32),
        ],
        compiler_params=pltpu.CompilerParams(vmem_limit_bytes=60 * 1024 * 1024),
        name="band",
    )(info, embed, flag_near, flag_far, limit, target, fwd, back, head, count)


def place(info_ref, b, o, rows, cols):
    return pl.multiple_of(b * rows + info_ref[0] * (info_ref[1] + o * cols), 128)


def windows_body(n_off, rows, cols, info_ref, tiles_ref, out_ref, line):
    n_enc, each, bins = tiles_ref.shape
    lead = 2 * EDGE
    line[...] = jnp.zeros(line.shape, F32)
    whole = jnp.concatenate(
        [tiles_ref[e].astype(F32) for e in range(n_enc)] + [jnp.zeros((each, 128), F32)], axis=1
    )
    line[:, : n_enc * bins + 128] = moved_right(whole, lead)
    for index in range(out_ref.shape[0]):
        start = place(info_ref, index // n_off, index % n_off, rows, cols)
        out_ref[index] = line[:, pl.ds(start, out_ref.shape[2])].astype(out_ref.dtype)


def windows(info, tiles, n_bin, n_off, rows, cols, wide):
    n_enc, each, bins = tiles.shape
    return pl.pallas_call(
        lambda *refs: windows_body(n_off, rows, cols, *refs),
        out_shape=jax.ShapeDtypeStruct((n_bin * n_off, each, wide), tiles.dtype),
        in_specs=[
            pl.BlockSpec(memory_space=pltpu.SMEM),
            pl.BlockSpec(memory_space=pltpu.VMEM),
        ],
        out_specs=pl.BlockSpec(memory_space=pltpu.VMEM),
        scratch_shapes=[
            pltpu.VMEM((each, (n_bin - 1) * rows + n_enc * n_off * cols + wide + 128), F32)
        ],
        name="windows",
    )(info, tiles)


def lines_body(n_off, rows, cols, wide, info_ref, parts_ref, out_ref, line):
    n_enc, each, total = out_ref.shape
    bins = total - (parts_ref.shape[2] - wide)
    line[...] = jnp.zeros(line.shape, F32)
    extra = parts_ref[0, :, wide:]
    for index in range(parts_ref.shape[0]):
        start = place(info_ref, index // n_off, index % n_off, rows, cols)
        line[:, pl.ds(start, wide)] += parts_ref[index, :, :wide]
        if index:
            extra = extra + parts_ref[index, :, wide:]
    for e in range(n_enc):
        out_ref[e, :, :bins] = line[:, e * bins : (e + 1) * bins]
        out_ref[e, :, bins:] = extra


def lines_of(info, parts, n_enc, n_off, bins, rows, cols, wide):
    group, each, total = parts.shape
    return pl.pallas_call(
        lambda *refs: lines_body(n_off, rows, cols, wide, *refs),
        out_shape=jax.ShapeDtypeStruct((n_enc, each, bins + total - wide), F32),
        in_specs=[
            pl.BlockSpec(memory_space=pltpu.SMEM),
            pl.BlockSpec(memory_space=pltpu.VMEM),
        ],
        out_specs=pl.BlockSpec(memory_space=pltpu.VMEM),
        scratch_shapes=[
            pltpu.VMEM((each, group // n_off * rows + n_enc * n_off * cols + wide), F32)
        ],
        name="lines",
    )(info, parts)


def shards(
    encoder_in,
    gain_enc,
    conv_one,
    proj_weight,
    conv_two,
    head_weight,
    target,
    valid_bins,
    offset_limit,
    dilations,
):
    chans, encoder_bins = encoder_in.shape
    width_in = conv_one.shape[2]
    second = conv_two.shape[1]
    rows, cols = target.shape
    n_enc, n_bin, n_off = (lax.axis_size(axis) for axis in EVERY)
    group = n_bin * n_off
    each = 2 * second // group
    length = valid_bins.shape[0]
    extent = cols * n_enc * n_off
    first_dilation = dilations[0]
    second_dilation = dilations[1]
    enc_id, bin_id, off_id = (lax.axis_index(axis) for axis in EVERY)
    row_start = bin_id * rows
    tile_id = enc_id * n_off + off_id
    offs_start = tile_id * cols

    activ = jax.nn.gelu(gain_enc[:, None] * encoder_in.astype(F32)).astype(BF16)
    framed = with_halo(activ, "enc", 1, HALO)
    framed_bins = encoder_bins + 2 * HALO
    everywhere = from_everyone(framed, GROUP).reshape(width_in, framed_bins)
    count = count_cells(valid_bins, offset_limit)
    goal = with_halo(target.T, "bin", 1, HALO)
    goal = with_halo(goal, ("enc", "off"), 0, HALO)

    weight_one = conv_one.reshape(3 * chans, width_in)
    taps = jnp.dot(weight_one, everywhere, preferred_element_type=F32)
    conv_out = sum(
        lax.dynamic_slice(
            taps, (tap * chans, HALO + (tap - 1) * first_dilation), (chans, encoder_bins)
        )
        for tap in range(3)
    )
    hidden = (encoder_in.astype(F32) + conv_out).astype(BF16)
    proj_rows = jnp.transpose(proj_weight, (0, 2, 1)).reshape(2 * second, chans)
    partial_embed = jnp.dot(proj_rows, hidden, preferred_element_type=F32)
    summed = exchange(partial_embed.reshape(group, each, encoder_bins), GROUP).sum(axis=0)
    tiles = from_everyone(summed.astype(BF16), "enc")
    wide = 512
    wide_far = 640
    is_far = (bin_id * n_off + off_id) * each >= second
    spots = jnp.stack([is_far.astype(jnp.int32), enc_id * n_off * cols]).astype(jnp.int32)
    embed = exchange(windows(spots, tiles, n_bin, n_off, rows, cols, wide_far), GROUP)
    embed = embed.reshape(2 * second, wide_far)
    flags = jnp.pad(valid_bins.astype(F32), (2 * EDGE, extent + wide_far))[None]
    flag_near = lax.dynamic_slice_in_dim(flags, row_start + EDGE, wide, 1)
    flag_far = lax.dynamic_slice_in_dim(flags, row_start + offs_start, wide_far, 1)
    limits = jnp.pad(offset_limit.astype(F32), (EDGE, wide))[None]
    limit = lax.dynamic_slice_in_dim(limits, row_start, wide, 1)
    goal = jnp.pad(goal.astype(F32), ((0, 0), (HALO, wide - rows - 3 * HALO)))
    info = jnp.stack(
        [second_dilation, offs_start, row_start, jnp.int32(extent), jnp.int32(length)]
    ).astype(jnp.int32)
    taps_two = conv_two.reshape(3, 3, second, second)
    fwd = jnp.transpose(taps_two, (1, 3, 0, 2)).reshape(3 * second, 3 * second)
    back = jnp.transpose(taps_two, (1, 2, 0, 3)).reshape(3 * second, 3 * second)
    pred, near_grad, far_grad, band_grad, error = band(
        info,
        embed,
        flag_near,
        flag_far,
        limit,
        goal,
        fwd,
        back,
        head_weight[:, None],
        count,
        rows,
        cols,
    )
    prediction = pred.T

    size = 9 * second * second
    share = size // group
    pad_share = -(-(share + 1) // (each * 128)) * 128
    extra = jnp.concatenate(
        [band_grad.reshape(group, share), jnp.broadcast_to(error[0:1, 0:1], (group, 1))], axis=1
    )
    extra = jnp.pad(extra, ((0, 0), (0, each * pad_share - share - 1)))
    parts = jnp.concatenate(
        [jnp.pad(near_grad, ((0, 0), (0, wide - rows))), far_grad], axis=0
    ).reshape(group, each, wide)
    parts = jnp.concatenate([parts, extra.reshape(group, each, pad_share)], axis=2)
    parts = lines_of(
        spots, exchange(parts, GROUP), n_enc, n_off, encoder_bins, rows, cols, wide
    )
    parts = exchange(parts, "enc").sum(axis=0)
    grad_embed = parts[:, :encoder_bins].astype(BF16).astype(F32)
    gathered = from_everyone(
        jnp.concatenate([grad_embed, parts[:, encoder_bins:]], axis=1), GROUP
    )
    grad_rows = gathered[:, :, :encoder_bins].reshape(2 * second, encoder_bins).astype(BF16)
    extra = gathered[:, :, encoder_bins:].reshape(group, each * pad_share)
    grad_conv_two = (
        extra[:, :share]
        .reshape(3, second, 3, second)
        .transpose(0, 2, 1, 3)
        .reshape(9, second, second)
    )
    loss_mean = extra[0, share : share + 1] / (1.0 + count[0, 0:1])

    dhidden = jnp.dot(proj_rows.T, grad_rows, preferred_element_type=F32).astype(BF16)
    proj_local = lax.dot_general(
        hidden, grad_rows, (((1,), (1,)), ((), ())), preferred_element_type=F32
    )
    proj_local = jnp.transpose(proj_local.reshape(chans, 2, second), (1, 0, 2))
    shifted = jnp.concatenate(
        [
            lax.dynamic_update_slice(
                jnp.zeros((chans, framed_bins), BF16),
                dhidden,
                (0, HALO + (tap - 1) * first_dilation),
            )
            for tap in range(3)
        ],
        axis=0,
    )
    conv_local = lax.dot_general(
        shifted, everywhere, (((1,), (1,)), ((), ())), preferred_element_type=F32
    )
    own_width = width_in // n_enc
    conv_size = 3 * chans * own_width
    proj_size = 2 * chans * second
    conv_local = jnp.transpose(
        conv_local.reshape(3 * chans, n_enc, own_width), (1, 0, 2)
    ).reshape(n_enc, conv_size // 128, 128)
    common = proj_local.reshape(proj_size // 128, 128)
    final = exchange(
        jnp.concatenate(
            [conv_local, jnp.broadcast_to(common[None], (n_enc, *common.shape))], axis=1
        ),
        "enc",
    ).sum(axis=0)
    grad_conv_one = final[: conv_size // 128].reshape(3, chans, own_width)
    grad_proj = final[conv_size // 128 :].reshape(2, chans, second)
    return (prediction, loss_mean, grad_conv_two, grad_proj, grad_conv_one)


def solution(mesh):
    in_specs = (
        P(("bin", "off"), "enc"),
        P(("bin", "off")),
        P(None, ("bin", "off"), None),
        P(None, ("bin", "off"), None),
        P(),
        P(),
        P("bin", ("enc", "off")),
        P(),
        P(),
        P(),
    )
    out_specs = (
        P("bin", ("enc", "off")),
        P(),
        P(),
        P(None, ("bin", "off"), None),
        P(None, ("bin", "off"), "enc"),
    )
    return jax.shard_map(shards, mesh=mesh, in_specs=in_specs, out_specs=out_specs, check_vma=False)
```

```python
import jax
import jax.numpy as jnp
from jax import lax
from jax.experimental import pallas as pl
from jax.experimental.pallas import tpu as pltpu
from jax.sharding import PartitionSpec as P

LARGEST_DILATION = 8
HALO = LARGEST_DILATION
EDGE = 2 * LARGEST_DILATION
F32 = jnp.float32
BF16 = jnp.bfloat16
MASKED = -1e38
GROUP = ("bin", "off")
EVERY = ("enc", "bin", "off")


def with_halo(cells, axis, dim, width):
    count = lax.axis_size(axis)
    ends = count - 1
    head = lax.slice_in_dim(cells, 0, width, axis=dim)
    tail = lax.slice_in_dim(cells, cells.shape[dim] - width, cells.shape[dim], axis=dim)
    return jnp.concatenate(
        [
            lax.ppermute(tail, axis, [(i, (i + 1) % count) for i in range(ends)]),
            cells,
            lax.ppermute(head, axis, [((i + 1) % count, i) for i in range(ends)]),
        ],
        axis=dim,
    )


def exchange(array, axis):
    return lax.all_to_all(array, axis, 0, 0, tiled=True)


def from_everyone(array, axis):
    return exchange(jnp.broadcast_to(array[None], (lax.axis_size(axis), *array.shape)), axis)


def pieces(x, shift):
    return [
        pltpu.roll(x[:, start : start + 128], shift, 1) for start in range(0, x.shape[1], 128)
    ]


def moved_right(x, shift):
    parts = pieces(x, shift)
    edge = lax.broadcasted_iota(jnp.int32, parts[0].shape, 1) < shift
    return jnp.concatenate(
        [jnp.where(edge, parts[k - 1], parts[k]) for k in range(len(parts))], axis=1
    )


def moved_left(x, shift):
    parts = pieces(x, 128 - shift)
    edge = lax.broadcasted_iota(jnp.int32, parts[0].shape, 1) < 128 - shift
    return jnp.concatenate(
        [jnp.where(edge, parts[k], parts[(k + 1) % len(parts)]) for k in range(len(parts))],
        axis=1,
    )


def prep_body(flags_ref, square_ref, limit_ref, count_ref, flag_line, limit_line):
    total = limit_ref.shape[1]
    used = square_ref.shape[0]
    high = -(-(used + 1) // 16) * 16
    square = jnp.concatenate(
        [square_ref[...].astype(F32), jnp.zeros((high - used, 128), F32)], axis=0
    ).astype(BF16)
    place = lax.broadcasted_iota(jnp.int32, (128, 128), 0)
    other = lax.broadcasted_iota(jnp.int32, (128, 128), 1)
    row_h = lax.broadcasted_iota(jnp.int32, (high, high), 0)
    col_h = lax.broadcasted_iota(jnp.int32, (high, high), 1)
    inner = jnp.dot(
        square, jnp.where(place < other, 1.0, 0.0).astype(BF16), preferred_element_type=F32
    )
    outer = jnp.dot(
        jnp.where(col_h < row_h, 1.0, 0.0).astype(BF16), square, preferred_element_type=F32
    )
    table = inner + jnp.sum(outer, axis=1, keepdims=True)
    table_hi = jnp.floor(table * (1.0 / 128.0))
    tables = jnp.concatenate([table_hi, table - 128.0 * table_hi], axis=1).astype(BF16)
    chunk = 512
    row_of = lax.broadcasted_iota(jnp.int32, (high, chunk), 0)
    lane_of = lax.broadcasted_iota(jnp.int32, (128, chunk), 0)
    ids = lax.broadcasted_iota(jnp.int32, (1, chunk), 1)
    acc = jnp.zeros((1, chunk), F32)
    for start in range(0, total, chunk):
        far = jnp.minimum(ids + start + limit_ref[:, start : start + chunk], total)
        picks = jnp.where(row_of == lax.shift_right_logical(far, 7), 1.0, 0.0).astype(BF16)
        found = lax.dot_general(
            tables, picks, (((0,), (0,)), ((), ())), preferred_element_type=F32
        )
        found = 128.0 * found[:128] + found[128:]
        inside = jnp.sum(jnp.where(lane_of == (far & 127), found, 0.0), axis=0, keepdims=True)
        acc = acc + flags_ref[:, start : start + chunk].astype(F32) * inside
    counted = jnp.sum(acc, axis=1, keepdims=True) - jnp.sum(
        jnp.sum(square.astype(F32) * table, axis=1, keepdims=True), axis=0, keepdims=True
    )
    count_ref[...] = jnp.broadcast_to(counted, count_ref.shape)
    flag_line[...] = jnp.zeros(flag_line.shape, F32)
    limit_line[...] = jnp.zeros(limit_line.shape, F32)
    flag_line[:, 128 : 128 + total] = flags_ref[...].astype(F32)
    limit_line[:, 128 : 128 + total] = limit_ref[...].astype(F32)


def prep(valid_bins, offset_limit, more):
    total = valid_bins.shape[0]
    return pl.pallas_call(
        prep_body,
        out_shape=(
            jax.ShapeDtypeStruct((8, 128), F32),
            jax.ShapeDtypeStruct((1, 128 + total + more), F32),
            jax.ShapeDtypeStruct((1, 128 + total + 512), F32),
        ),
        name="prep",
    )(valid_bins[None], valid_bins.reshape(total // 128, 128), offset_limit[None])


def band_body(
    info_ref,
    embed_ref,
    flag_ref,
    limit_ref,
    target_ref,
    fwd_ref,
    back_ref,
    head_ref,
    count_ref,
    pred_ref,
    sums_out,
    grad_out,
    lines,
    parts,
    dress,
    owns,
    weights,
    goals,
):
    wide = goals.shape[1]
    chans = embed_ref.shape[0] // 2
    cols, rows = pred_ref.shape
    steps = cols + 2 * EDGE
    first_mid, last_mid = HALO, steps - HALO
    dilation = info_ref[0]
    offs_start = info_ref[1]
    row_start = info_ref[2]
    extent = info_ref[3]
    length = info_ref[4]
    wide_far = embed_ref.shape[1]
    turn = 448
    lane = lax.broadcasted_iota(jnp.int32, (1, wide), 1)
    bins = row_start + jnp.where(lane < turn, lane, lane - wide)
    near = jnp.where(
        (bins >= 0) & (bins < length), moved_left(moved_left(embed_ref[:chans].astype(F32), EDGE)[:, :wide], EDGE), MASKED
    )
    near_of = (
        moved_right(near, dilation).astype(BF16),
        near.astype(BF16),
        moved_left(near, dilation).astype(BF16),
    )

    def around(ref, start):
        start = pl.multiple_of(start, 128)
        before = ref[:, pl.ds(start, 128)]
        body = ref[:, pl.ds(pl.multiple_of(start + 128, 128), wide)]
        last = jnp.where(lane[:, :128] < turn % 128, body[:, wide - 128 :], before)
        return jnp.broadcast_to(
            jnp.concatenate([body[:, : wide - 128], last], axis=1), (8, wide)
        )

    flag_near = around(flag_ref, row_start)
    limit = around(limit_ref, row_start)
    goals[...] = jnp.zeros(goals.shape, F32)
    goals[:, : target_ref.shape[1]] = target_ref[...].astype(F32)
    goals[...] = moved_left(goals[...], HALO)
    far = moved_left(embed_ref[chans:].astype(F32), HALO).astype(BF16)
    flags = flag_ref[:, pl.ds(pl.multiple_of(row_start + offs_start, 128), wide_far + 128)]
    flags = moved_left(
        jnp.broadcast_to(flags, (8, wide_far + 128)), 128 - 2 * EDGE + HALO
    )[:, :wide_far]
    tiles = wide // 128
    tiles_far = wide_far // 128
    lane_tile = lax.broadcasted_iota(jnp.int32, (chans, 128), 1)
    before_turn = lane_tile < turn % 128

    def shifted(rolled, shift, extra, last_only):
        keep = last_only < 128 - shift

        def part(k):
            return jnp.where(keep, rolled[k % tiles_far], rolled[(k + 1) % tiles_far])

        out = [part(k + extra) for k in range(tiles)]
        out[-1] = jnp.where(last_only < turn % 128, out[-1], part(tiles + extra))
        return jnp.concatenate(out, axis=1)

    def make_line(shift, extra):
        turned = (128 - shift) & 127
        rolled = pieces(far, turned)
        rolled_flags = pieces(flags, turned)
        for more in range(extra):
            u = shift + 128 * more
            lines[u] = shifted(rolled, shift, more, lane_tile)
            flag = shifted(rolled_flags, shift, more, lane_tile[:8])
            offset = offs_start + u - HALO - EDGE
            offset = jnp.where(offset >= 0, offset, extent).astype(F32)
            weights[u] = jnp.where(limit > offset, flag_near * flag, 0.0)

    total_lines = steps + 2 * HALO
    both = total_lines - 128

    @pl.loop(0, both, unroll=16)
    def _(shift):
        make_line(shift, 2)

    @pl.loop(both, 128, unroll=16)
    def _(shift):
        make_line(shift, 1)

    def act_of(t, tap, width):
        line = lines[t + HALO + (tap - 1) * dilation, :, :width]
        return jnp.maximum(near_of[tap][:, :width] + line, jnp.zeros((), BF16))

    fwd = fwd_ref[...]

    @pl.loop(0, steps, unroll=40)
    def _(t):
        stacked = jnp.concatenate([act_of(t, tap, wide) for tap in range(3)], axis=0)
        parts[t] = jnp.dot(fwd, stacked, preferred_element_type=F32)

    @pl.when(offs_start == 0)
    def _():
        @pl.loop(0, EDGE)
        def _(t):
            parts[t] = jnp.zeros((3 * chans, wide), F32)

    @pl.when(offs_start + cols == extent)
    def _():
        @pl.loop(steps - EDGE, steps)
        def _(t):
            parts[t] = jnp.zeros((3 * chans, wide), F32)

    owns[:EDGE] = jnp.zeros((EDGE, chans, rows), BF16)
    owns[steps - EDGE :] = jnp.zeros((EDGE, chans, rows), BF16)
    head = jnp.broadcast_to(head_ref[...], (chans, wide))
    scale = 2.0 / (1.0 + count_ref[0:1, 0:1])

    def make_dres(t, err, own):
        conv = (
            parts[t - dilation, :chans]
            + parts[t, chans : 2 * chans]
            + parts[t + dilation, 2 * chans :]
        )
        resid = (near + lines[t + HALO].astype(F32)) + conv
        pred = jnp.sum(head * jnp.maximum(resid, 0.0), axis=0, keepdims=True)
        differ = pred - goals[pl.ds(t - HALO, 1)]
        weighted = weights[t + HALO, 0:1] * differ
        dres = jnp.where(resid > 0.0, head * (weighted * scale), 0.0).astype(BF16)
        dress[t] = dres
        if own:
            owns[t] = dres[:, :rows]
            pred_ref[pl.ds(t - EDGE, 1)] = pred[:, :rows]
            err = err + (weighted * differ)[:, :rows]
        return err

    err = jnp.zeros((1, rows), F32)
    err = lax.fori_loop(first_mid, EDGE, lambda t, e: make_dres(t, e, False), err, unroll=4)
    err = lax.fori_loop(EDGE, steps - EDGE, lambda t, e: make_dres(t, e, True), err, unroll=8)
    err = lax.fori_loop(
        steps - EDGE, last_mid, lambda t, e: make_dres(t, e, False), err, unroll=4
    )
    err = jnp.broadcast_to(jnp.sum(err, axis=1, keepdims=True), (1, 128))
    back = back_ref[...]

    @pl.loop(first_mid, last_mid, unroll=72)
    def _(t):
        dres = dress[t]
        stacked = jnp.concatenate(
            [
                moved_left(dres, dilation)[:, :rows],
                dres[:, :rows],
                moved_right(dres, dilation)[:, :rows],
            ],
            axis=0,
        )
        parts[t, :, :rows] = jnp.dot(back, stacked, preferred_element_type=F32)

    bunch = 8

    def make_grads(n, carry):
        near_sum, far_sum = carry
        far_sum = moved_right(far_sum, bunch)
        for k in range(bunch):
            t = steps - EDGE - bunch - n * bunch + k
            dact = (
                parts[t + dilation, :chans, :rows]
                + parts[t, chans : 2 * chans, :rows]
                + parts[t - dilation, 2 * chans :, :rows]
            )
            act = act_of(t, 1, rows).astype(F32)
            dpair = owns[t].astype(F32) + jnp.where(act > 0.0, dact, 0.0)
            near_sum = near_sum + dpair
            dpair = jnp.concatenate([dpair, jnp.zeros((chans, wide - rows), F32)], axis=1)
            far_sum = far_sum + (moved_right(dpair, k) if k else dpair)
        return near_sum, far_sum

    near_sum, far_sum = lax.fori_loop(
        0,
        cols // bunch,
        make_grads,
        (jnp.zeros((chans, rows), F32), jnp.zeros((chans, wide), F32)),
    )
    group, each, _ = sums_out.shape
    sums_out[...] = jnp.zeros(sums_out.shape, F32)
    for first in range(0, chans, each):
        sums_out[first // each, :, :rows] = near_sum[first : first + each]
        sums_out[(chans + first) // each, :, :wide] = far_sum[first : first + each]
    grad_out[...] = jnp.zeros((3 * chans, 3 * chans), F32)

    def add_weight_grads(first, batch):
        left = jnp.concatenate(
            [
                jnp.concatenate([act_of(first + k, tap, rows) for tap in range(3)], axis=0)
                for k in range(batch)
            ],
            axis=1,
        )
        right = jnp.concatenate(
            [
                jnp.concatenate([owns[first + k + move * dilation] for k in range(batch)], axis=1)
                for move in (1, 0, -1)
            ],
            axis=0,
        )
        grad_out[...] += lax.dot_general(
            left, right, (((1,), (1,)), ((), ())), preferred_element_type=F32
        )

    batch = 32

    @pl.loop(0, cols // batch)
    def _(n):
        add_weight_grads(EDGE + n * batch, batch)

    @pl.when(offs_start > 0)
    def _():
        add_weight_grads(first_mid, HALO)

    @pl.when(offs_start + cols < extent)
    def _():
        add_weight_grads(steps - EDGE, HALO)

    total = grad_out[...]
    size = 3 * chans
    for index in range(group):
        first = 3 * index
        sums_out[index, 0:1, wide : wide + size] = total[first : first + 1]
        sums_out[index, 0:1, wide + 128 : wide + 128 + size] = total[first + 1 : first + 2]
        sums_out[index, 1:2, wide : wide + size] = total[first + 2 : first + 3]
        sums_out[index, 1:2, wide + 128 :] = err


def band(info, embed, flag_line, limit_line, target, fwd, back, head, count, rows, cols, group):
    chans = embed.shape[0] // 2
    wide = 512
    steps = cols + 2 * EDGE
    vmem = pl.BlockSpec(memory_space=pltpu.VMEM)
    return pl.pallas_call(
        band_body,
        out_shape=(
            jax.ShapeDtypeStruct((cols, rows), F32),
            jax.ShapeDtypeStruct((group, 2 * chans // group, wide + 256), F32),
        ),
        in_specs=[pl.BlockSpec(memory_space=pltpu.SMEM)] + [vmem] * 8,
        out_specs=(vmem,) * 2,
        scratch_shapes=[
            pltpu.VMEM((3 * chans, 3 * chans), F32),
            pltpu.VMEM((steps + 2 * HALO, chans, wide), BF16),
            pltpu.VMEM((steps, 3 * chans, wide), F32),
            pltpu.VMEM((steps, chans, wide), BF16),
            pltpu.VMEM((steps, chans, rows), BF16),
            pltpu.VMEM((steps + 2 * HALO, 8, wide), F32),
            pltpu.VMEM((steps - 2 * HALO, wide), F32),
        ],
        compiler_params=pltpu.CompilerParams(vmem_limit_bytes=60 * 1024 * 1024),
        name="band",
    )(info, embed, flag_line, limit_line, target, fwd, back, head, count)


def place(info_ref, b, o, rows, cols):
    return pl.multiple_of(b * rows + info_ref[5] * (info_ref[6] + o * cols), 128)


def windows_body(n_off, rows, cols, info_ref, tiles_ref, out_ref, line):
    n_enc, each, bins = tiles_ref.shape
    lead = 2 * EDGE
    line[...] = jnp.zeros(line.shape, F32)
    whole = jnp.concatenate(
        [tiles_ref[e].astype(F32) for e in range(n_enc)] + [jnp.zeros((each, 128), F32)], axis=1
    )
    line[:, : n_enc * bins + 128] = moved_right(whole, lead)
    for index in range(out_ref.shape[0]):
        start = place(info_ref, index // n_off, index % n_off, rows, cols)
        out_ref[index] = line[:, pl.ds(start, out_ref.shape[2])].astype(out_ref.dtype)


def windows(info, tiles, n_bin, n_off, rows, cols, wide):
    n_enc, each, bins = tiles.shape
    return pl.pallas_call(
        lambda *refs: windows_body(n_off, rows, cols, *refs),
        out_shape=jax.ShapeDtypeStruct((n_bin * n_off, each, wide), tiles.dtype),
        in_specs=[
            pl.BlockSpec(memory_space=pltpu.SMEM),
            pl.BlockSpec(memory_space=pltpu.VMEM),
        ],
        out_specs=pl.BlockSpec(memory_space=pltpu.VMEM),
        scratch_shapes=[
            pltpu.VMEM((each, (n_bin - 1) * rows + n_enc * n_off * cols + wide + 128), F32)
        ],
        name="windows",
    )(info, tiles)


def lines_body(n_off, rows, cols, wide, info_ref, parts_ref, out_ref, line):
    n_enc, each, total = out_ref.shape
    bins = total - (parts_ref.shape[2] - wide)
    line[...] = jnp.zeros(line.shape, F32)
    extra = parts_ref[0, :, wide:]
    for index in range(parts_ref.shape[0]):
        start = place(info_ref, index // n_off, index % n_off, rows, cols)
        line[:, pl.ds(start, wide)] += parts_ref[index, :, :wide]
        if index:
            extra = extra + parts_ref[index, :, wide:]
    for e in range(n_enc):
        out_ref[e, :, :bins] = line[:, e * bins : (e + 1) * bins]
        out_ref[e, :, bins:] = extra


def lines_of(info, parts, n_enc, n_off, bins, rows, cols, wide):
    group, each, total = parts.shape
    return pl.pallas_call(
        lambda *refs: lines_body(n_off, rows, cols, wide, *refs),
        out_shape=jax.ShapeDtypeStruct((n_enc, each, bins + total - wide), F32),
        in_specs=[
            pl.BlockSpec(memory_space=pltpu.SMEM),
            pl.BlockSpec(memory_space=pltpu.VMEM),
        ],
        out_specs=pl.BlockSpec(memory_space=pltpu.VMEM),
        scratch_shapes=[
            pltpu.VMEM((each, group // n_off * rows + n_enc * n_off * cols + wide), F32)
        ],
        name="lines",
    )(info, parts)


def shards(
    encoder_in,
    gain_enc,
    conv_one,
    proj_weight,
    conv_two,
    head_weight,
    target,
    valid_bins,
    offset_limit,
    dilations,
):
    chans, encoder_bins = encoder_in.shape
    width_in = conv_one.shape[2]
    second = conv_two.shape[1]
    rows, cols = target.shape
    n_enc, n_bin, n_off = (lax.axis_size(axis) for axis in EVERY)
    group = n_bin * n_off
    each = 2 * second // group
    length = valid_bins.shape[0]
    extent = cols * n_enc * n_off
    first_dilation = dilations[0]
    second_dilation = dilations[1]
    enc_id, bin_id, off_id = (lax.axis_index(axis) for axis in EVERY)
    row_start = bin_id * rows
    tile_id = enc_id * n_off + off_id
    offs_start = tile_id * cols

    activ = jax.nn.gelu(gain_enc[:, None] * encoder_in.astype(F32)).astype(BF16)
    framed = with_halo(activ, "enc", 1, HALO)
    framed_bins = encoder_bins + 2 * HALO
    everywhere = from_everyone(framed, GROUP).reshape(width_in, framed_bins)
    wide = 512
    wide_far = 640
    count, flag_line, limit_line = prep(valid_bins, offset_limit, extent + wide_far)
    is_far = (bin_id * n_off + off_id) * each >= second
    values = (
        second_dilation,
        offs_start,
        row_start,
        extent,
        length,
        is_far.astype(jnp.int32),
        enc_id * n_off * cols,
    )
    slot = jnp.arange(8, dtype=jnp.int32)
    info = sum(jnp.where(slot == index, value, 0) for index, value in enumerate(values))
    info = info.astype(jnp.int32)
    goal = with_halo(target, "bin", 0, HALO).T
    everywhere, goal, count, flag_line, limit_line, info = lax.optimization_barrier(
        (everywhere, goal, count, flag_line, limit_line, info)
    )
    goal = with_halo(goal, ("enc", "off"), 0, HALO)

    weight_one = conv_one.reshape(3 * chans, width_in)
    taps = jnp.dot(weight_one, everywhere, preferred_element_type=F32)
    conv_out = sum(
        lax.dynamic_slice(
            taps, (tap * chans, HALO + (tap - 1) * first_dilation), (chans, encoder_bins)
        )
        for tap in range(3)
    )
    hidden = (encoder_in.astype(F32) + conv_out).astype(BF16)
    proj_rows = jnp.transpose(proj_weight, (0, 2, 1)).reshape(2 * second, chans)
    partial_embed = jnp.dot(proj_rows, hidden, preferred_element_type=F32)
    summed = exchange(partial_embed.reshape(group, each, encoder_bins), GROUP)
    summed = summed.sum(axis=0)
    tiles = from_everyone(summed.astype(BF16), "enc")
    tiles, conv_two, head_weight = lax.optimization_barrier((tiles, conv_two, head_weight))
    embed = exchange(windows(info, tiles, n_bin, n_off, rows, cols, wide_far), GROUP)
    embed = embed.reshape(2 * second, wide_far)
    taps_two = conv_two.reshape(3, 3, second, second)
    fwd = jnp.transpose(taps_two, (1, 3, 0, 2)).reshape(3 * second, 3 * second)
    back = jnp.transpose(taps_two, (1, 2, 0, 3)).reshape(3 * second, 3 * second)
    pred, parts = band(
        info,
        embed,
        flag_line,
        limit_line,
        goal,
        fwd,
        back,
        head_weight[:, None],
        count,
        rows,
        cols,
        group,
    )
    prediction = pred.T

    parts = lines_of(
        info, exchange(parts, GROUP), n_enc, n_off, encoder_bins, rows, cols, wide
    )
    parts = exchange(parts, "enc").sum(axis=0)
    grad_embed = parts[:, :encoder_bins].astype(BF16).astype(F32)
    gathered = from_everyone(
        jnp.concatenate([grad_embed, parts[:, encoder_bins:]], axis=1), GROUP
    )
    grad_rows = gathered[:, :, :encoder_bins].reshape(2 * second, encoder_bins).astype(BF16)
    extra = gathered[:, :, encoder_bins:]
    grad_conv_two = jnp.stack(
        [extra[:, 0, : 3 * second], extra[:, 0, 128 : 128 + 3 * second], extra[:, 1, : 3 * second]],
        axis=1,
    )
    grad_conv_two = (
        grad_conv_two.reshape(3, second, 3, second)
        .transpose(0, 2, 1, 3)
        .reshape(9, second, second)
    )
    loss_mean = extra[0, 1, 128:129] / (1.0 + count[0, 0:1])

    dhidden = jnp.dot(proj_rows.T, grad_rows, preferred_element_type=F32).astype(BF16)
    proj_local = lax.dot_general(
        hidden, grad_rows, (((1,), (1,)), ((), ())), preferred_element_type=F32
    )
    proj_local = jnp.transpose(proj_local.reshape(chans, 2, second), (1, 0, 2))
    shifted = jnp.concatenate(
        [
            lax.dynamic_update_slice(
                jnp.zeros((chans, framed_bins), BF16),
                dhidden,
                (0, HALO + (tap - 1) * first_dilation),
            )
            for tap in range(3)
        ],
        axis=0,
    )
    conv_local = lax.dot_general(
        shifted, everywhere, (((1,), (1,)), ((), ())), preferred_element_type=F32
    )
    own_width = width_in // n_enc
    conv_size = 3 * chans * own_width
    proj_size = 2 * chans * second
    conv_local = jnp.transpose(
        conv_local.reshape(3 * chans, n_enc, own_width), (1, 0, 2)
    ).reshape(n_enc, conv_size // 128, 128)
    common = proj_local.reshape(proj_size // 128, 128)
    final = exchange(
        jnp.concatenate(
            [conv_local, jnp.broadcast_to(common[None], (n_enc, *common.shape))], axis=1
        ),
        "enc",
    ).sum(axis=0)
    grad_conv_one = final[: conv_size // 128].reshape(3, chans, own_width)
    grad_proj = final[conv_size // 128 :].reshape(2, chans, second)
    return (prediction, loss_mean, grad_conv_two, grad_proj, grad_conv_one)


def solution(mesh):
    in_specs = (
        P(("bin", "off"), "enc"),
        P(("bin", "off")),
        P(None, ("bin", "off"), None),
        P(None, ("bin", "off"), None),
        P(),
        P(),
        P("bin", ("enc", "off")),
        P(),
        P(),
        P(),
    )
    out_specs = (
        P("bin", ("enc", "off")),
        P(),
        P(),
        P(None, ("bin", "off"), None),
        P(None, ("bin", "off"), "enc"),
    )
    return jax.shard_map(shards, mesh=mesh, in_specs=in_specs, out_specs=out_specs, check_vma=False)
```

```python
import jax
import jax.numpy as jnp
from jax import lax
from jax.experimental import pallas as pl
from jax.experimental.pallas import tpu as pltpu
from jax.sharding import PartitionSpec as P

LARGEST_DILATION = 8
HALO = LARGEST_DILATION
EDGE = 2 * LARGEST_DILATION
F32 = jnp.float32
BF16 = jnp.bfloat16
MASKED = -1e38
GROUP = ("bin", "off")
EVERY = ("enc", "bin", "off")


def with_halo(cells, axis, dim, width):
    count = lax.axis_size(axis)
    ends = count - 1
    head = lax.slice_in_dim(cells, 0, width, axis=dim)
    tail = lax.slice_in_dim(cells, cells.shape[dim] - width, cells.shape[dim], axis=dim)
    return jnp.concatenate(
        [
            lax.ppermute(tail, axis, [(i, (i + 1) % count) for i in range(ends)]),
            cells,
            lax.ppermute(head, axis, [((i + 1) % count, i) for i in range(ends)]),
        ],
        axis=dim,
    )


def exchange(array, axis):
    return lax.all_to_all(array, axis, 0, 0, tiled=True)


def from_everyone(array, axis):
    return exchange(jnp.broadcast_to(array[None], (lax.axis_size(axis), *array.shape)), axis)


def pieces(x, shift):
    return [
        pltpu.roll(x[:, start : start + 128], shift, 1) for start in range(0, x.shape[1], 128)
    ]


def moved_right(x, shift):
    parts = pieces(x, shift)
    edge = lax.broadcasted_iota(jnp.int32, parts[0].shape, 1) < shift
    return jnp.concatenate(
        [jnp.where(edge, parts[k - 1], parts[k]) for k in range(len(parts))], axis=1
    )


def moved_left(x, shift):
    parts = pieces(x, 128 - shift)
    edge = lax.broadcasted_iota(jnp.int32, parts[0].shape, 1) < 128 - shift
    return jnp.concatenate(
        [jnp.where(edge, parts[k], parts[(k + 1) % len(parts)]) for k in range(len(parts))],
        axis=1,
    )


def prep_body(flags_ref, square_ref, limit_ref, count_ref, flag_line, limit_line):
    total = limit_ref.shape[1]
    used = square_ref.shape[0]
    high = -(-(used + 1) // 16) * 16
    square = jnp.concatenate(
        [square_ref[...].astype(F32), jnp.zeros((high - used, 128), F32)], axis=0
    ).astype(BF16)
    place = lax.broadcasted_iota(jnp.int32, (128, 128), 0)
    other = lax.broadcasted_iota(jnp.int32, (128, 128), 1)
    row_h = lax.broadcasted_iota(jnp.int32, (high, high), 0)
    col_h = lax.broadcasted_iota(jnp.int32, (high, high), 1)
    inner = jnp.dot(
        square, jnp.where(place < other, 1.0, 0.0).astype(BF16), preferred_element_type=F32
    )
    outer = jnp.dot(
        jnp.where(col_h < row_h, 1.0, 0.0).astype(BF16), square, preferred_element_type=F32
    )
    table = inner + jnp.sum(outer, axis=1, keepdims=True)
    table_hi = jnp.floor(table * (1.0 / 128.0))
    tables = jnp.concatenate([table_hi, table - 128.0 * table_hi], axis=1).astype(BF16)
    chunk = 512
    row_of = lax.broadcasted_iota(jnp.int32, (high, chunk), 0)
    lane_of = lax.broadcasted_iota(jnp.int32, (128, chunk), 0)
    ids = lax.broadcasted_iota(jnp.int32, (1, chunk), 1)
    acc = jnp.zeros((1, chunk), F32)
    for start in range(0, total, chunk):
        far = jnp.minimum(ids + start + limit_ref[:, start : start + chunk], total)
        picks = jnp.where(row_of == lax.shift_right_logical(far, 7), 1.0, 0.0).astype(BF16)
        found = lax.dot_general(
            tables, picks, (((0,), (0,)), ((), ())), preferred_element_type=F32
        )
        found = 128.0 * found[:128] + found[128:]
        inside = jnp.sum(jnp.where(lane_of == (far & 127), found, 0.0), axis=0, keepdims=True)
        acc = acc + flags_ref[:, start : start + chunk].astype(F32) * inside
    counted = jnp.sum(acc, axis=1, keepdims=True) - jnp.sum(
        jnp.sum(square.astype(F32) * table, axis=1, keepdims=True), axis=0, keepdims=True
    )
    count_ref[...] = jnp.broadcast_to(counted, count_ref.shape)
    flag_line[...] = jnp.zeros(flag_line.shape, F32)
    limit_line[...] = jnp.zeros(limit_line.shape, F32)
    flag_line[:, 128 : 128 + total] = flags_ref[...].astype(F32)
    limit_line[:, 128 : 128 + total] = limit_ref[...].astype(F32)


def prep(valid_bins, offset_limit, more):
    total = valid_bins.shape[0]
    return pl.pallas_call(
        prep_body,
        out_shape=(
            jax.ShapeDtypeStruct((8, 128), F32),
            jax.ShapeDtypeStruct((1, 128 + total + more), F32),
            jax.ShapeDtypeStruct((1, 128 + total + 512), F32),
        ),
        name="prep",
    )(valid_bins[None], valid_bins.reshape(total // 128, 128), offset_limit[None])


def band_body(
    info_ref,
    embed_ref,
    flag_ref,
    limit_ref,
    target_ref,
    fwd_ref,
    back_ref,
    head_ref,
    count_ref,
    pred_ref,
    sums_out,
    grad_out,
    lines,
    parts,
    dress,
    owns,
    weights,
    goals,
):
    wide = goals.shape[1]
    chans = embed_ref.shape[0] // 2
    cols, rows = pred_ref.shape
    steps = cols + 2 * EDGE
    first_mid, last_mid = HALO, steps - HALO
    dilation = info_ref[0]
    offs_start = info_ref[1]
    row_start = info_ref[2]
    extent = info_ref[3]
    length = info_ref[4]
    wide_far = embed_ref.shape[1]
    turn = 448
    lane = lax.broadcasted_iota(jnp.int32, (1, wide), 1)
    bins = row_start + jnp.where(lane < turn, lane, lane - wide)
    near = jnp.where(
        (bins >= 0) & (bins < length), moved_left(moved_left(embed_ref[:chans].astype(F32), EDGE)[:, :wide], EDGE), MASKED
    )
    near_of = (
        moved_right(near, dilation).astype(BF16),
        near.astype(BF16),
        moved_left(near, dilation).astype(BF16),
    )

    def around(ref, start):
        start = pl.multiple_of(start, 128)
        before = ref[:, pl.ds(start, 128)]
        body = ref[:, pl.ds(pl.multiple_of(start + 128, 128), wide)]
        last = jnp.where(lane[:, :128] < turn % 128, body[:, wide - 128 :], before)
        return jnp.broadcast_to(
            jnp.concatenate([body[:, : wide - 128], last], axis=1), (8, wide)
        )

    flag_near = around(flag_ref, row_start)
    limit = around(limit_ref, row_start)
    goals[...] = jnp.zeros(goals.shape, F32)
    goals[:, : target_ref.shape[1]] = target_ref[...].astype(F32)
    goals[...] = moved_left(goals[...], HALO)
    far = moved_left(embed_ref[chans:].astype(F32), HALO).astype(BF16)
    flags = flag_ref[:, pl.ds(pl.multiple_of(row_start + offs_start, 128), wide_far + 128)]
    flags = moved_left(
        jnp.broadcast_to(flags, (8, wide_far + 128)), 128 - 2 * EDGE + HALO
    )[:, :wide_far]
    tiles = wide // 128
    tiles_far = wide_far // 128
    lane_tile = lax.broadcasted_iota(jnp.int32, (chans, 128), 1)
    before_turn = lane_tile < turn % 128

    def shifted(rolled, shift, extra, last_only):
        keep = last_only < 128 - shift

        def part(k):
            return jnp.where(keep, rolled[k % tiles_far], rolled[(k + 1) % tiles_far])

        out = [part(k + extra) for k in range(tiles)]
        out[-1] = jnp.where(last_only < turn % 128, out[-1], part(tiles + extra))
        return jnp.concatenate(out, axis=1)

    def make_line(shift, extra):
        turned = (128 - shift) & 127
        rolled = pieces(far, turned)
        rolled_flags = pieces(flags, turned)
        for more in range(extra):
            u = shift + 128 * more
            lines[u] = shifted(rolled, shift, more, lane_tile)
            flag = shifted(rolled_flags, shift, more, lane_tile[:8])
            offset = offs_start + u - HALO - EDGE
            offset = jnp.where(offset >= 0, offset, extent).astype(F32)
            weights[u] = jnp.where(limit > offset, flag_near * flag, 0.0)

    total_lines = steps + 2 * HALO
    both = total_lines - 128

    @pl.loop(0, both, unroll=16)
    def _(shift):
        make_line(shift, 2)

    @pl.loop(both, 128, unroll=16)
    def _(shift):
        make_line(shift, 1)

    def act_of(t, tap, width):
        line = lines[t + HALO + (tap - 1) * dilation, :, :width]
        return jnp.maximum(near_of[tap][:, :width] + line, jnp.zeros((), BF16))

    fwd = fwd_ref[...]

    @pl.loop(0, steps, unroll=40)
    def _(t):
        stacked = jnp.concatenate([act_of(t, tap, wide) for tap in range(3)], axis=0)
        parts[t] = jnp.dot(fwd, stacked, preferred_element_type=F32)

    @pl.when(offs_start == 0)
    def _():
        @pl.loop(0, EDGE)
        def _(t):
            parts[t] = jnp.zeros((3 * chans, wide), F32)

    @pl.when(offs_start + cols == extent)
    def _():
        @pl.loop(steps - EDGE, steps)
        def _(t):
            parts[t] = jnp.zeros((3 * chans, wide), F32)

    owns[:EDGE] = jnp.zeros((EDGE, chans, rows), BF16)
    owns[steps - EDGE :] = jnp.zeros((EDGE, chans, rows), BF16)
    head = jnp.broadcast_to(head_ref[...], (chans, wide))
    scale = 2.0 / (1.0 + count_ref[0:1, 0:1])

    def make_dres(t, err, own):
        conv = (
            parts[t - dilation, :chans]
            + parts[t, chans : 2 * chans]
            + parts[t + dilation, 2 * chans :]
        )
        resid = (near + lines[t + HALO].astype(F32)) + conv
        pred = jnp.sum(head * jnp.maximum(resid, 0.0), axis=0, keepdims=True)
        differ = pred - goals[pl.ds(t - HALO, 1)]
        weighted = weights[t + HALO, 0:1] * differ
        dres = jnp.where(resid > 0.0, head * (weighted * scale), 0.0).astype(BF16)
        dress[t] = dres
        if own:
            owns[t] = dres[:, :rows]
            pred_ref[pl.ds(t - EDGE, 1)] = pred[:, :rows]
            err = err + (weighted * differ)[:, :rows]
        return err

    err = jnp.zeros((1, rows), F32)
    err = lax.fori_loop(first_mid, EDGE, lambda t, e: make_dres(t, e, False), err, unroll=4)
    err = lax.fori_loop(EDGE, steps - EDGE, lambda t, e: make_dres(t, e, True), err, unroll=8)
    err = lax.fori_loop(
        steps - EDGE, last_mid, lambda t, e: make_dres(t, e, False), err, unroll=4
    )
    err = jnp.broadcast_to(jnp.sum(err, axis=1, keepdims=True), (1, 128))
    back = back_ref[...]

    @pl.loop(first_mid, last_mid, unroll=72)
    def _(t):
        dres = dress[t]
        stacked = jnp.concatenate(
            [
                moved_left(dres, dilation)[:, :rows],
                dres[:, :rows],
                moved_right(dres, dilation)[:, :rows],
            ],
            axis=0,
        )
        parts[t, :, :rows] = jnp.dot(back, stacked, preferred_element_type=F32)

    bunch = 8

    def make_grads(n, carry):
        near_sum, far_sum = carry
        far_sum = moved_right(far_sum, bunch)
        for k in range(bunch):
            t = steps - EDGE - bunch - n * bunch + k
            dact = (
                parts[t + dilation, :chans, :rows]
                + parts[t, chans : 2 * chans, :rows]
                + parts[t - dilation, 2 * chans :, :rows]
            )
            act = act_of(t, 1, rows).astype(F32)
            dpair = owns[t].astype(F32) + jnp.where(act > 0.0, dact, 0.0)
            near_sum = near_sum + dpair
            dpair = jnp.concatenate([dpair, jnp.zeros((chans, wide - rows), F32)], axis=1)
            far_sum = far_sum + (moved_right(dpair, k) if k else dpair)
        return near_sum, far_sum

    near_sum, far_sum = lax.fori_loop(
        0,
        cols // bunch,
        make_grads,
        (jnp.zeros((chans, rows), F32), jnp.zeros((chans, wide), F32)),
    )
    group, each, _ = sums_out.shape
    sums_out[...] = jnp.zeros(sums_out.shape, F32)
    for first in range(0, chans, each):
        sums_out[first // each, :, :rows] = near_sum[first : first + each]
        sums_out[(chans + first) // each, :, :wide] = far_sum[first : first + each]
    grad_out[...] = jnp.zeros((3 * chans, 3 * chans), F32)

    def add_weight_grads(first, batch):
        left = jnp.concatenate(
            [
                jnp.concatenate([act_of(first + k, tap, rows) for tap in range(3)], axis=0)
                for k in range(batch)
            ],
            axis=1,
        )
        right = jnp.concatenate(
            [
                jnp.concatenate([owns[first + k + move * dilation] for k in range(batch)], axis=1)
                for move in (1, 0, -1)
            ],
            axis=0,
        )
        grad_out[...] += lax.dot_general(
            left, right, (((1,), (1,)), ((), ())), preferred_element_type=F32
        )

    batch = 32

    @pl.loop(0, cols // batch)
    def _(n):
        add_weight_grads(EDGE + n * batch, batch)

    @pl.when(offs_start > 0)
    def _():
        add_weight_grads(first_mid, HALO)

    @pl.when(offs_start + cols < extent)
    def _():
        add_weight_grads(steps - EDGE, HALO)

    total = grad_out[...]
    size = 3 * chans
    for index in range(group):
        first = 3 * index
        sums_out[index, 0:1, wide : wide + size] = total[first : first + 1]
        sums_out[index, 0:1, wide + 128 : wide + 128 + size] = total[first + 1 : first + 2]
        sums_out[index, 1:2, wide : wide + size] = total[first + 2 : first + 3]
        sums_out[index, 1:2, wide + 128 :] = err


def band(info, embed, flag_line, limit_line, target, fwd, back, head, count, rows, cols, group):
    chans = embed.shape[0] // 2
    wide = 512
    steps = cols + 2 * EDGE
    vmem = pl.BlockSpec(memory_space=pltpu.VMEM)
    return pl.pallas_call(
        band_body,
        out_shape=(
            jax.ShapeDtypeStruct((cols, rows), F32),
            jax.ShapeDtypeStruct((group, 2 * chans // group, wide + 256), F32),
        ),
        in_specs=[pl.BlockSpec(memory_space=pltpu.SMEM)] + [vmem] * 8,
        out_specs=(vmem,) * 2,
        scratch_shapes=[
            pltpu.VMEM((3 * chans, 3 * chans), F32),
            pltpu.VMEM((steps + 2 * HALO, chans, wide), BF16),
            pltpu.VMEM((steps, 3 * chans, wide), F32),
            pltpu.VMEM((steps, chans, wide), BF16),
            pltpu.VMEM((steps, chans, rows), BF16),
            pltpu.VMEM((steps + 2 * HALO, 8, wide), F32),
            pltpu.VMEM((steps - 2 * HALO, wide), F32),
        ],
        compiler_params=pltpu.CompilerParams(vmem_limit_bytes=60 * 1024 * 1024),
        name="band",
    )(info, embed, flag_line, limit_line, target, fwd, back, head, count)


def place(info_ref, b, o, rows, cols):
    return pl.multiple_of(b * rows + info_ref[5] * (info_ref[6] + o * cols), 128)


def windows_body(n_off, rows, cols, info_ref, tiles_ref, out_ref, line):
    n_enc, each, bins = tiles_ref.shape
    lead = 2 * EDGE
    line[...] = jnp.zeros(line.shape, F32)
    whole = jnp.concatenate(
        [tiles_ref[e].astype(F32) for e in range(n_enc)] + [jnp.zeros((each, 128), F32)], axis=1
    )
    line[:, : n_enc * bins + 128] = moved_right(whole, lead)
    for index in range(out_ref.shape[0]):
        start = place(info_ref, index // n_off, index % n_off, rows, cols)
        out_ref[index] = line[:, pl.ds(start, out_ref.shape[2])].astype(out_ref.dtype)


def windows(info, tiles, n_bin, n_off, rows, cols, wide):
    n_enc, each, bins = tiles.shape
    return pl.pallas_call(
        lambda *refs: windows_body(n_off, rows, cols, *refs),
        out_shape=jax.ShapeDtypeStruct((n_bin * n_off, each, wide), tiles.dtype),
        in_specs=[
            pl.BlockSpec(memory_space=pltpu.SMEM),
            pl.BlockSpec(memory_space=pltpu.VMEM),
        ],
        out_specs=pl.BlockSpec(memory_space=pltpu.VMEM),
        scratch_shapes=[
            pltpu.VMEM((each, (n_bin - 1) * rows + n_enc * n_off * cols + wide + 128), F32)
        ],
        name="windows",
    )(info, tiles)


def lines_body(n_off, rows, cols, wide, info_ref, parts_ref, out_ref, line):
    n_enc, each, total = out_ref.shape
    bins = total - (parts_ref.shape[2] - wide)
    line[...] = jnp.zeros(line.shape, F32)
    extra = parts_ref[0, :, wide:]
    for index in range(parts_ref.shape[0]):
        start = place(info_ref, index // n_off, index % n_off, rows, cols)
        line[:, pl.ds(start, wide)] += parts_ref[index, :, :wide]
        if index:
            extra = extra + parts_ref[index, :, wide:]
    for e in range(n_enc):
        out_ref[e, :, :bins] = line[:, e * bins : (e + 1) * bins]
        out_ref[e, :, bins:] = extra


def lines_of(info, parts, n_enc, n_off, bins, rows, cols, wide):
    group, each, total = parts.shape
    return pl.pallas_call(
        lambda *refs: lines_body(n_off, rows, cols, wide, *refs),
        out_shape=jax.ShapeDtypeStruct((n_enc, each, bins + total - wide), F32),
        in_specs=[
            pl.BlockSpec(memory_space=pltpu.SMEM),
            pl.BlockSpec(memory_space=pltpu.VMEM),
        ],
        out_specs=pl.BlockSpec(memory_space=pltpu.VMEM),
        scratch_shapes=[
            pltpu.VMEM((each, group // n_off * rows + n_enc * n_off * cols + wide), F32)
        ],
        name="lines",
    )(info, parts)


def shards(
    encoder_in,
    gain_enc,
    conv_one,
    proj_weight,
    conv_two,
    head_weight,
    target,
    valid_bins,
    offset_limit,
    dilations,
):
    chans, encoder_bins = encoder_in.shape
    width_in = conv_one.shape[2]
    second = conv_two.shape[1]
    rows, cols = target.shape
    n_enc, n_bin, n_off = (lax.axis_size(axis) for axis in EVERY)
    group = n_bin * n_off
    each = 2 * second // group
    length = valid_bins.shape[0]
    extent = cols * n_enc * n_off
    first_dilation = dilations[0]
    second_dilation = dilations[1]
    enc_id, bin_id, off_id = (lax.axis_index(axis) for axis in EVERY)
    row_start = bin_id * rows
    tile_id = enc_id * n_off + off_id
    offs_start = tile_id * cols

    activ = jax.nn.gelu(gain_enc[:, None] * encoder_in.astype(F32)).astype(BF16)
    framed = with_halo(activ, "enc", 1, HALO)
    framed_bins = encoder_bins + 2 * HALO
    everywhere = from_everyone(framed, GROUP).reshape(width_in, framed_bins)
    wide = 512
    wide_far = 640
    count, flag_line, limit_line = prep(valid_bins, offset_limit, extent + wide_far)
    is_far = (bin_id * n_off + off_id) * each >= second
    values = (
        second_dilation,
        offs_start,
        row_start,
        extent,
        length,
        is_far.astype(jnp.int32),
        enc_id * n_off * cols,
    )
    slot = jnp.arange(8, dtype=jnp.int32)
    info = sum(jnp.where(slot == index, value, 0) for index, value in enumerate(values))
    info = info.astype(jnp.int32)
    goal = with_halo(target, "bin", 0, HALO).T
    everywhere, goal = lax.optimization_barrier((everywhere, goal))

    weight_one = conv_one.reshape(3 * chans, width_in)
    taps = jnp.dot(weight_one, everywhere, preferred_element_type=F32)
    conv_out = sum(
        lax.dynamic_slice(
            taps, (tap * chans, HALO + (tap - 1) * first_dilation), (chans, encoder_bins)
        )
        for tap in range(3)
    )
    hidden = (encoder_in.astype(F32) + conv_out).astype(BF16)
    proj_rows = jnp.transpose(proj_weight, (0, 2, 1)).reshape(2 * second, chans)
    partial_embed = jnp.dot(proj_rows, hidden, preferred_element_type=F32)
    summed = exchange(partial_embed.reshape(group, each, encoder_bins), GROUP)
    summed, goal, count, flag_line, limit_line, info = lax.optimization_barrier(
        (summed, goal, count, flag_line, limit_line, info)
    )
    goal = with_halo(goal, ("enc", "off"), 0, HALO)
    summed = summed.sum(axis=0)
    tiles = from_everyone(summed.astype(BF16), "enc")
    tiles, conv_two, head_weight = lax.optimization_barrier((tiles, conv_two, head_weight))
    embed = exchange(windows(info, tiles, n_bin, n_off, rows, cols, wide_far), GROUP)
    embed = embed.reshape(2 * second, wide_far)
    taps_two = conv_two.reshape(3, 3, second, second)
    fwd = jnp.transpose(taps_two, (1, 3, 0, 2)).reshape(3 * second, 3 * second)
    back = jnp.transpose(taps_two, (1, 2, 0, 3)).reshape(3 * second, 3 * second)
    pred, parts = band(
        info,
        embed,
        flag_line,
        limit_line,
        goal,
        fwd,
        back,
        head_weight[:, None],
        count,
        rows,
        cols,
        group,
    )
    prediction = pred.T

    parts = lines_of(
        info, exchange(parts, GROUP), n_enc, n_off, encoder_bins, rows, cols, wide
    )
    parts = exchange(parts, "enc").sum(axis=0)
    grad_embed = parts[:, :encoder_bins].astype(BF16).astype(F32)
    gathered = from_everyone(
        jnp.concatenate([grad_embed, parts[:, encoder_bins:]], axis=1), GROUP
    )
    grad_rows = gathered[:, :, :encoder_bins].reshape(2 * second, encoder_bins).astype(BF16)
    extra = gathered[:, :, encoder_bins:]
    grad_conv_two = jnp.stack(
        [extra[:, 0, : 3 * second], extra[:, 0, 128 : 128 + 3 * second], extra[:, 1, : 3 * second]],
        axis=1,
    )
    grad_conv_two = (
        grad_conv_two.reshape(3, second, 3, second)
        .transpose(0, 2, 1, 3)
        .reshape(9, second, second)
    )
    loss_mean = extra[0, 1, 128:129] / (1.0 + count[0, 0:1])

    dhidden = jnp.dot(proj_rows.T, grad_rows, preferred_element_type=F32).astype(BF16)
    proj_local = lax.dot_general(
        hidden, grad_rows, (((1,), (1,)), ((), ())), preferred_element_type=F32
    )
    proj_local = jnp.transpose(proj_local.reshape(chans, 2, second), (1, 0, 2))
    shifted = jnp.concatenate(
        [
            lax.dynamic_update_slice(
                jnp.zeros((chans, framed_bins), BF16),
                dhidden,
                (0, HALO + (tap - 1) * first_dilation),
            )
            for tap in range(3)
        ],
        axis=0,
    )
    conv_local = lax.dot_general(
        shifted, everywhere, (((1,), (1,)), ((), ())), preferred_element_type=F32
    )
    own_width = width_in // n_enc
    conv_size = 3 * chans * own_width
    proj_size = 2 * chans * second
    conv_local = jnp.transpose(
        conv_local.reshape(3 * chans, n_enc, own_width), (1, 0, 2)
    ).reshape(n_enc, conv_size // 128, 128)
    common = proj_local.reshape(proj_size // 128, 128)
    final = exchange(
        jnp.concatenate(
            [conv_local, jnp.broadcast_to(common[None], (n_enc, *common.shape))], axis=1
        ),
        "enc",
    ).sum(axis=0)
    grad_conv_one = final[: conv_size // 128].reshape(3, chans, own_width)
    grad_proj = final[conv_size // 128 :].reshape(2, chans, second)
    return (prediction, loss_mean, grad_conv_two, grad_proj, grad_conv_one)


def solution(mesh):
    in_specs = (
        P(("bin", "off"), "enc"),
        P(("bin", "off")),
        P(None, ("bin", "off"), None),
        P(None, ("bin", "off"), None),
        P(),
        P(),
        P("bin", ("enc", "off")),
        P(),
        P(),
        P(),
    )
    out_specs = (
        P("bin", ("enc", "off")),
        P(),
        P(),
        P(None, ("bin", "off"), None),
        P(None, ("bin", "off"), "enc"),
    )
    return jax.shard_map(shards, mesh=mesh, in_specs=in_specs, out_specs=out_specs, check_vma=False)
```
